32 devices in a mesh: parts: 2 (over x), cluster: 16 (over z, y, core).
Axes of the slice: x: 2, y: 2, z: 4, core: 2. Of those that a mesh axis runs over, the one named last changes fastest.
Arguments:
- queries: float32 [4096, 1024], P(('parts', 'cluster')), parts along dimension 0, may hold values from -1 to 1
- passages: float32 [64, 128, 1024], P(('parts', 'cluster')), parts along dimension 0, may hold values from -6 to 6
- first_blocks: int32 [4096, 4], P(('parts', 'cluster')), parts along dimension 0, may hold values from 0 to 31, all different within a row; in each aligned block of 128 rows (0 to 127, 128 to 255, ...) at most 24 rows name the same one
- followup_blocks: int32 [4096, 4], P(('parts', 'cluster')), parts along dimension 0, may hold values from 0 to 31, all different within a row; in each aligned block of 128 rows (0 to 127, 128 to 255, ...) at most 24 rows name the same one
Outputs:
- expanded: float32 [4096, 1024], P(('parts', 'cluster')), parts along dimension 0
- second_scores: float32 [4096, 4, 128], P(('parts', 'cluster')), parts along dimension 0
The draws below stay inside these ranges and needn't reach their ends.
There are 2 independent parts, one for each index of `parts`. The reference program is written for one: setup_inputs(seed, part) draws one part's arguments, and reference() takes and returns one part's arrays. A program takes and returns all parts, laid end to end along the dimension named above; each array names one. Nothing has to cross between parts.
Inputs may be any that keep to these rules, and one draw needn't show every extreme that they name: `first_blocks`: each row names 4 different blocks; among the queries of one device no block is named more than 24 times, and some block is named exactly 24 times. `followup_blocks`: each row names 4 different blocks; among the queries of one device no block is named more than 24 times, and some block is named exactly 24 times.
All inputs are finite; a program needn't handle non-finite values.
Results may differ from the reference program's by a relative error of at most 0.00014.
Values sent between devices are 32-bit elements; how exact they have to be, the bound alone decides.
A program may use at most 128 MiB of HBM per device.

```python
import math
from functools import partial
import jax
import jax.numpy as jnp
import numpy as np
from jax import lax

E = 1024
ROWS = 128
KB = 4
Q_DEV = 128
NBLK = 32
QUERIES = 2048
CAP = 24


def draw_queries(key, part):
    bound = float((E + 160) // E)
    base = jax.random.normal(jax.random.fold_in(key, 7002), (QUERIES, E), jnp.float32) * E ** (-0.5)
    return jnp.clip(base, -bound, bound)


def draw_passages(key, part):
    noise = jax.random.normal(jax.random.fold_in(key, 7005), (NBLK, ROWS, E), jnp.float32)
    values = noise
    return jnp.clip(values, -6.0, 6.0)


def shared_out(own_key, own, number, rows, count, top, most, slope):
    order = jax.random.permutation(own_key, count)
    crowded, usual = shares(count, rows * top, most, slope, True), shares(count, rows * top, most, slope, False)
    places = jnp.arange(count)

    def named(sizes, offset_by):
        used = int((sizes > 0).sum())
        fixed = max(1, used // 4)
        moved = fixed + (places - fixed + offset_by * (used - fixed)) % max(1, count - fixed)
        return jnp.zeros((count,), jnp.int32).at[order[jnp.where(places < fixed, places, moved)]].set(jnp.asarray(sizes, jnp.int32))

    sizes = jnp.where(number % 4 == 0, named(crowded, number // 4), named(usual, number - number // 4 - 1))
    mixed = jax.random.permutation(jax.random.fold_in(own, 3), count)
    donor, receiver = mixed[0:count // 2 * 2:2], mixed[1:count // 2 * 2:2]
    margin = jnp.minimum(sizes[donor] - 1, most - sizes[receiver]) // 2
    margin = jnp.where((donor == order[0]) | (receiver == order[0]) | (sizes[receiver] == 0), 0, jnp.maximum(margin, 0))
    moved = jax.random.randint(jax.random.fold_in(own, 4), (count // 2,), 0, 1 << 20) % (margin + 1)
    sizes = sizes.at[donor].add(-moved).at[receiver].add(moved)
    members = jnp.searchsorted(jnp.cumsum(sizes), jnp.arange(rows * top), side="right").astype(jnp.int32)
    grid = members.reshape(top, rows).T
    grid = grid[jax.random.permutation(jax.random.fold_in(own, 1), rows)]
    offset_by = jax.random.randint(jax.random.fold_in(own, 2), (rows, 1), 0, top)
    return jnp.take_along_axis(grid, (jnp.arange(top)[None, :] + offset_by) % top, axis=1)


def shares(number_of, total, reach, slope, full):
    loads = [(1 << 20) // math.isqrt(rank ** slope) + 1 for rank in range(1, number_of + 1)]
    largest = reach if full else min(reach, max(-(-total // number_of), total * loads[0] // sum(loads)))
    least = 1 if total - largest >= number_of - 1 else 0
    holding, spare = [largest] + [least] * (number_of - 1), total - largest - least * (number_of - 1)
    while spare > 0:
        free = [i for i in range(1, number_of) if holding[i] < largest] or [i for i in range(1, number_of) if holding[i] < reach]
        pool, budget = sum([loads[i] for i in free]), spare
        for i in free:
            more = min(reach - holding[i], max(1, budget * loads[i] // pool), spare)
            holding[i] = holding[i] + more
            spare = spare - more
    return np.array(holding)


def setup_inputs(seed: int = 0, part: int = 0) -> dict:
    key_list = jax.random.split(jax.random.key(seed), 5)
    own_keys = jax.random.split(jax.random.fold_in(key_list[4], part), 5)
    queries = draw_queries(jax.random.fold_in(jax.random.fold_in(key_list[4], part), 71), part)
    passages = draw_passages(jax.random.fold_in(jax.random.fold_in(key_list[4], part), 71), part)
    first_blocks_keys = jax.random.split(jax.random.fold_in(own_keys[2], 1), QUERIES // Q_DEV)
    first_blocks_turns = jax.random.permutation(jax.random.fold_in(own_keys[2], 3), QUERIES // Q_DEV)
    first_blocks = jax.vmap(lambda own, number: shared_out(jax.random.fold_in(own_keys[2], 2), own, number, Q_DEV, NBLK, KB, CAP, 2))(first_blocks_keys, first_blocks_turns).reshape((QUERIES, KB))
    followup_blocks_keys = jax.random.split(jax.random.fold_in(own_keys[3], 1), QUERIES // Q_DEV)
    followup_blocks_turns = jax.random.permutation(jax.random.fold_in(own_keys[3], 3), QUERIES // Q_DEV)
    followup_blocks = jax.vmap(lambda own, number: shared_out(jax.random.fold_in(own_keys[3], 2), own, number, Q_DEV, NBLK, KB, CAP, 2))(followup_blocks_keys, followup_blocks_turns).reshape((QUERIES, KB))
    return {"queries": queries, "passages": passages, "first_blocks": first_blocks, "followup_blocks": followup_blocks}


SOFTMAX_HEAT = 2.0
FEEDBACK = 0.5


def one_group(packed, passages):
    cluster_query_rows, group_first, group_second = packed
    initial_round_rows = passages[group_first]
    match_scores = SOFTMAX_HEAT * jnp.einsum("dt,dbzt->dbz", cluster_query_rows, initial_round_rows, precision=lax.Precision.HIGHEST)
    flat_scores = match_scores.reshape(match_scores.shape[0], -1)
    weights = jax.nn.softmax(flat_scores, axis=1).reshape(match_scores.shape)
    feedback = jnp.einsum("gkr,gkre->ge", weights, initial_round_rows, precision=lax.Precision.HIGHEST)
    expanded = cluster_query_rows + (FEEDBACK * cluster_query_rows.shape[1] ** -0.5) * feedback
    second_rows = passages[group_second]
    second = jnp.einsum("dt,dbzt->dbz", expanded, second_rows, precision=lax.Precision.HIGHEST)
    return expanded, second


def reference(queries, passages, first_blocks, followup_blocks):
    groups = queries.shape[0] // 64
    packed = (queries.reshape(groups, 64, -1), first_blocks.reshape(groups, 64, -1), followup_blocks.reshape(groups, 64, -1))
    expanded, second = lax.map(partial(one_group, passages=passages), packed)
    return expanded.reshape(queries.shape), second.reshape(queries.shape[0], first_blocks.shape[1], -1)
```

```python
import functools

import jax
import jax.numpy as jnp
from jax import lax
from jax.experimental import pallas as pl
from jax.experimental.pallas import tpu as pltpu
from jax.sharding import PartitionSpec as P

SOFTMAX_HEAT = 2.0
FEEDBACK = 0.5
MASKED = -1e30
VMEM_BYTES = 60 * 1024 * 1024


def position_targets(block_ids, capacity):
    flat_ids = block_ids.reshape(-1)
    matches = flat_ids[:, None] == flat_ids[None, :]
    positions = jnp.arange(flat_ids.shape[0], dtype=jnp.int32)
    earlier = positions[None, :] < positions[:, None]
    ranking = jnp.sum(jnp.logical_and(matches, earlier), axis=1, dtype=jnp.int32)
    return flat_ids * capacity + ranking


def pack_rows(values, targets, owners, resident_blocks, capacity):
    buffer = jnp.zeros((owners * resident_blocks * capacity, values.shape[1]), values.dtype)
    buffer = buffer.at[targets].set(values)
    return buffer.reshape(owners, resident_blocks, capacity, values.shape[1])


def reply(results):
    return (
        lax.all_to_all(results[0], "cluster", split_axis=0, concat_axis=0, tiled=True),
        lax.all_to_all(results[1], "cluster", split_axis=0, concat_axis=0, tiled=True),
        lax.all_to_all(results[2], "cluster", split_axis=0, concat_axis=0, tiled=True),
    )


def send_back(match_scores):
    return lax.all_to_all(match_scores, "cluster", split_axis=0, concat_axis=0, tiled=True)


def local(queries, passages, first_blocks, followup_blocks):
    owners = lax.axis_size("cluster")
    resident_blocks = passages.shape[0]
    embed_width = queries.shape[1]
    per_query = first_blocks.shape[1]
    pair_count = queries.shape[0] * per_query
    all_blocks = owners * resident_blocks
    capacity = max(2, (3 * pair_count + 2 * all_blocks - 1) // (2 * all_blocks))
    coefficient = FEEDBACK * embed_width ** (-0.5)
    highest = lax.Precision.HIGHEST

    def project_onto_centroid(arrived):
        return jnp.einsum("nbce,bre->nbcr", arrived, passages, precision=highest)

    first_targets = position_targets(first_blocks, capacity)
    second_targets = position_targets(followup_blocks, capacity)
    repeated = jnp.repeat(queries, per_query, axis=0)
    first_sent = pack_rows(repeated, first_targets, owners, resident_blocks, capacity)
    match_scores = SOFTMAX_HEAT * project_onto_centroid(
        lax.all_to_all(first_sent, "cluster", split_axis=0, concat_axis=0, tiled=True)
    )
    highs = jnp.max(match_scores, axis=3)
    weights = jnp.exp(match_scores - highs[..., None])
    totals = jnp.sum(weights, axis=3)
    vectors = jnp.einsum("nbcr,bre->nbce", weights, passages, precision=highest)
    highs, totals, vectors = reply((highs, totals, vectors))
    highs = highs.reshape(-1)[first_targets].reshape(-1, per_query)
    totals = totals.reshape(-1)[first_targets].reshape(-1, per_query)
    vectors = vectors.reshape(-1, embed_width)[first_targets].reshape(-1, per_query, embed_width)
    peak_high = jnp.max(highs, axis=1, keepdims=True)
    scaled = jnp.exp(highs - peak_high)
    denominator = jnp.sum(scaled * totals, axis=1)
    feedback = jnp.einsum("qk,qke->qe", scaled, vectors, precision=highest) / denominator[:, None]
    expanded = queries + coefficient * feedback
    expanded_sent = pack_rows(
        jnp.repeat(expanded, per_query, axis=0), second_targets, owners, resident_blocks, capacity
    )
    returned = (lambda arrived: send_back(project_onto_centroid(arrived)))(
        lax.all_to_all(expanded_sent, "cluster", split_axis=0, concat_axis=0, tiled=True)
    )
    second_scores = returned.reshape(-1, returned.shape[3])[second_targets].reshape(
        queries.shape[0], per_query, -1
    )
    return (expanded, second_scores)


def dot_nt(a, b):
    return lax.dot_general(a, b, (((1,), (1,)), ((), ())), preferred_element_type=jnp.float32)


def dot_nn(a, b):
    return lax.dot_general(a, b, (((1,), (0,)), ((), ())), preferred_element_type=jnp.float32)


def halves(x):
    high = x.astype(jnp.bfloat16)
    return high, (x - high.astype(jnp.float32)).astype(jnp.bfloat16)


def ring_kernel(
    chips, queries, passages, first, followup, expanded, scores,
    corpus, corpus_hi, corpus_lo, pair, total, chosen, picked,
    load_sem, send_r, recv_r, send_l, recv_l, send_a, recv_a, send_b, recv_b,
):
    me = lax.axis_index("cluster")
    chip, core = me // 2, me % 2
    rows, width = queries.shape
    top = first.shape[1]
    size = passages.shape[1]
    half = chips // 2
    spot = (1 - chip % 2) * (chip // 2) + (chip % 2) * (chips - 1 - chip // 2)

    def chip_at(position):
        position = (position + chips) % chips
        late = position // half
        return (1 - late) * (2 * position) + late * (2 * (chips - 1 - position) + 1)

    right = 2 * chip_at(spot + 1) + core
    left = 2 * chip_at(spot + chips - 1) + core
    other = 2 * chip + 1 - core

    def remote(src, dst, send, recv, device):
        return pltpu.make_async_remote_copy(
            src_ref=src, dst_ref=dst, send_sem=send, recv_sem=recv,
            device_id={"cluster": device}, device_id_type=pl.DeviceIdType.MESH,
        )

    def rightward(step, src):
        return remote(src, corpus.at[step, 0], send_r.at[step], recv_r.at[step], right)

    def leftward(step, src):
        return remote(src, corpus.at[step, 1], send_l.at[step], recv_l.at[step], left)

    def across_a(step):
        return remote(corpus.at[step, 0], corpus.at[step, 2], send_a.at[step], recv_a.at[step], other)

    def across_b(step):
        return remote(corpus.at[step, 1], corpus.at[step, 3], send_b.at[step], recv_b.at[step], other)

    def blocks_of(step):
        away = (step + 1) // 2
        from_left = 2 * chip_at(spot + chips - away)
        from_right = 2 * chip_at(spot + away)
        a, b = (step + 1) % 2, step % 2
        return (
            (from_left + core) * 2 + a,
            (from_right + core) * 2 + b,
            (from_left + 1 - core) * 2 + a,
            (from_right + 1 - core) * 2 + b,
        )

    loads = (
        pltpu.make_async_copy(passages.at[1], corpus.at[0, 0], load_sem.at[0]),
        pltpu.make_async_copy(passages.at[0], corpus.at[0, 1], load_sem.at[1]),
    )
    for load in loads:
        load.start()
    barrier = pltpu.get_barrier_semaphore()
    for device in (right, left, other):
        pl.semaphore_signal(
            barrier, inc=1, device_id={"cluster": device}, device_id_type=pl.DeviceIdType.MESH
        )
    pl.semaphore_wait(barrier, 3)
    for load in loads:
        load.wait()
    rightward(1, corpus.at[0, 1]).start()
    leftward(1, corpus.at[0, 0]).start()

    def put_pair(x):
        high, low = halves(x)
        pair[pl.ds(0, rows), :] = high
        pair[pl.ds(rows, rows), :] = low

    put_pair(queries[...])
    total[...] = jnp.zeros_like(total)
    for j in range(top):
        column = followup[:, j : j + 1].astype(jnp.float32)
        chosen[j] = jnp.broadcast_to(column, (rows, size)).T
    picked[...] = jnp.zeros_like(picked)

    def first_round(step, carry):
        peak, norm = carry

        @pl.when(step > 0)
        def _():
            rightward(step, corpus.at[step, 0]).wait_recv()
            leftward(step, corpus.at[step, 1]).wait_recv()

        @pl.when(step < chips - 2)
        def _():
            rightward(step + 2, corpus.at[step, 0]).start()
            leftward(step + 2, corpus.at[step, 1]).start()

        across_a(step).start()
        across_b(step).start()
        across_a(step).wait_recv()
        across_b(step).wait_recv()

        for t in range(4):
            high, low = halves(corpus[step, t])
            corpus_hi[step, pl.ds(t * size, size), :] = high
            corpus_lo[step, pl.ds(t * size, size), :] = low
        both = dot_nt(pair[...], corpus_hi[step])
        found = SOFTMAX_HEAT * (
            both[:rows] + both[rows:] + dot_nt(pair[pl.ds(0, rows), :], corpus_lo[step])
        )
        parts, hits = [], []
        top_score = peak
        for t, block in enumerate(blocks_of(step)):
            hit = jnp.max(jnp.where(first[...] == block, 1.0, 0.0), axis=1, keepdims=True) > 0.0
            part = jnp.where(hit, found[:, t * size : (t + 1) * size], MASKED)
            top_score = jnp.maximum(top_score, jnp.max(part, axis=1, keepdims=True))
            parts.append(part)
            hits.append(hit)
        shrink = jnp.exp(peak - top_score)
        weights = jnp.concatenate(
            [jnp.where(hit, jnp.exp(part - top_score), 0.0) for hit, part in zip(hits, parts)], axis=1
        )
        norm = norm * shrink + jnp.sum(weights, axis=1, keepdims=True)
        high, low = halves(weights)
        mixed = dot_nn(jnp.concatenate([high, low], axis=0), corpus_hi[step])
        total[...] = total[...] * shrink + (
            mixed[:rows] + mixed[rows:] + dot_nn(high, corpus_lo[step])
        )
        return top_score, norm

    start = (jnp.full((rows, 1), MASKED, jnp.float32), jnp.zeros((rows, 1), jnp.float32))
    _, norm = lax.fori_loop(0, chips, first_round, start)

    after = queries[...] + (FEEDBACK * width ** (-0.5)) * (total[...] / norm)
    expanded[...] = after
    put_pair(after)

    def second_round(step, carry):
        both = dot_nt(corpus_hi[step], pair[...])
        found = both[:, :rows] + both[:, rows:] + dot_nt(corpus_lo[step], pair[pl.ds(0, rows), :])
        ids = [block.astype(jnp.float32) for block in blocks_of(step)]
        for j in range(top):
            names = chosen[j]
            value = picked[j]
            for t in range(4):
                value = jnp.where(names == ids[t], found[t * size : (t + 1) * size, :], value)
            picked[j] = value
        return carry

    lax.fori_loop(0, chips, second_round, 0)
    for j in range(top):
        scores[:, j, :] = picked[j].T

    def drain(step, carry):
        @pl.when(step > 0)
        def _():
            rightward(step, corpus.at[step, 0]).wait_send()
            leftward(step, corpus.at[step, 1]).wait_send()

        across_a(step).wait_send()
        across_b(step).wait_send()
        return carry

    lax.fori_loop(0, chips, drain, 0)


def ring_fits(queries, passages, first_blocks):
    owners = lax.axis_size("cluster")
    resident, size, width = passages.shape
    rows = queries.shape[0]
    corpus = owners * resident * size * width * 8
    rest = (5 * rows * width + 3 * first_blocks.shape[1] * rows * size) * 4
    return owners % 4 == 0 and resident == 2 and corpus + 2 * rest < VMEM_BYTES and rows == size


def device_program(queries, passages, first_blocks, followup_blocks):
    if not ring_fits(queries, passages, first_blocks):
        return local(queries, passages, first_blocks, followup_blocks)
    chips = lax.axis_size("cluster") // 2
    rows, width = queries.shape
    size = passages.shape[1]
    top = first_blocks.shape[1]
    vmem = pl.BlockSpec(memory_space=pltpu.VMEM)
    return pl.pallas_call(
        functools.partial(ring_kernel, chips),
        out_shape=(
            jax.ShapeDtypeStruct((rows, width), jnp.float32),
            jax.ShapeDtypeStruct((rows, top, size), jnp.float32),
        ),
        in_specs=[vmem, pl.BlockSpec(memory_space=pl.ANY), vmem, vmem],
        out_specs=(vmem, vmem),
        scratch_shapes=[
            pltpu.VMEM((chips, 4, size, width), jnp.float32),
            pltpu.VMEM((chips, 4 * size, width), jnp.bfloat16),
            pltpu.VMEM((chips, 4 * size, width), jnp.bfloat16),
            pltpu.VMEM((2 * rows, width), jnp.bfloat16),
            pltpu.VMEM((rows, width), jnp.float32),
            pltpu.VMEM((top, size, rows), jnp.float32),
            pltpu.VMEM((top, size, rows), jnp.float32),
            pltpu.SemaphoreType.DMA((2,)),
        ]
        + [pltpu.SemaphoreType.DMA((chips,))] * 8,
        compiler_params=pltpu.CompilerParams(
            collective_id=0, has_side_effects=True, vmem_limit_bytes=VMEM_BYTES
        ),
    )(queries, passages, first_blocks, followup_blocks)


def solution(mesh):
    return jax.shard_map(
        device_program,
        mesh=mesh,
        in_specs=(
            P(("parts", "cluster"), None),
            P(("parts", "cluster"), None, None),
            P(("parts", "cluster"), None),
            P(("parts", "cluster"), None),
        ),
        out_specs=(P(("parts", "cluster"), None), P(("parts", "cluster"), None, None)),
        check_vma=False,
    )
```
